16 devices in a mesh: dp: 2 (over z), sp: 8 (over y, x, core).
Axes of the slice: x: 2, y: 2, z: 2, core: 2. Of those that a mesh axis runs over, the one named last changes fastest.
Arguments:
- x_in: bfloat16 [16, 1024, 2048], P('dp', 'sp'), parts along dimension 0
- grad_y: bfloat16 [16, 1024, 2048], P('dp', 'sp'), parts along dimension 0
- positions: int32 [16, 1024], P('dp', 'sp'), parts along dimension 0
- g_norm: bfloat16 [2048], replicated
- w_query: bfloat16 [2048, 2048], replicated
- w_key: bfloat16 [2048, 2048], replicated
- w_value: bfloat16 [2048, 2048], replicated
- w_out: bfloat16 [2048, 2048], replicated
- g_query: bfloat16 [2048], replicated
- g_key: bfloat16 [2048], replicated
Outputs:
- output 1: bfloat16 [16, 1024, 2048], P('dp', 'sp'), parts along dimension 0
- output 2: bfloat16 [16, 1024, 2048], P('dp', 'sp'), parts along dimension 0
- output 3: float32 [4096], P(('dp', 'sp')), parts along dimension 0
- output 4: float32 [4096, 2048], P(('dp', 'sp')), parts along dimension 0
- output 5: float32 [4096, 2048], P(('dp', 'sp')), parts along dimension 0
- output 6: float32 [4096, 2048], P(('dp', 'sp')), parts along dimension 0
- output 7: float32 [4096, 2048], P(('dp', 'sp')), parts along dimension 0
- output 8: float32 [4096], P(('dp', 'sp')), parts along dimension 0
- output 9: float32 [4096], P(('dp', 'sp')), parts along dimension 0
There are 2 independent parts. The reference program is written for one: setup_inputs(seed, part) draws one part's arguments, and reference() takes and returns one part's arrays. A program takes and returns all parts, laid end to end along the dimension named above; an argument that names none is the same for every part.
All inputs are finite; a program needn't handle non-finite values.
Results may differ from the reference program's by a relative error of at most 0.0114602.
Values are sent between devices in bfloat16 or wider.
A program may use at most 1 GiB of HBM per device.

```python
import jax
import jax.numpy as jnp
from jax import lax

N_BATCH = 8
SEQ_LEN = 1024
D_MODEL = 2048
N_HEADS = 16
HEAD_DIM = 128
QUERY_BLOCK = min(128, SEQ_LEN)
NORM_EPS = 1e-5
ROPE_BASE = 10000.0
NEG_BIG = -1e30


def setup_inputs(seed: int = 0, part: int = 0) -> dict:
    part_key = jax.random.fold_in(jax.random.key(seed), part)
    key_x, key_dy, key_pos = jax.random.split(part_key, 3)
    weight_keys = jax.random.split(jax.random.key(seed + 1), 9)
    act_shape = (N_BATCH, SEQ_LEN, D_MODEL)
    x_in = jax.random.normal(key_x, act_shape, jnp.float32).astype(jnp.bfloat16)
    grad_y = jax.random.normal(key_dy, act_shape, jnp.float32).astype(jnp.bfloat16)
    tok_idx = jnp.arange(SEQ_LEN, dtype=jnp.int32)
    restart = jax.random.randint(key_pos, (N_BATCH, SEQ_LEN), 0, 256) == 0
    doc_start = lax.cummax(jnp.where(restart, tok_idx[None, :], 0), axis=1)
    positions = (tok_idx[None, :] - doc_start).astype(jnp.int32)
    fan_scale = D_MODEL ** -0.5
    head_q = jnp.repeat(jax.random.uniform(weight_keys[0], (N_HEADS,), jnp.float32, 0.5, 1.5), HEAD_DIM)
    head_k = jnp.repeat(jax.random.uniform(weight_keys[1], (N_HEADS,), jnp.float32, 0.5, 1.5), HEAD_DIM)
    w_shape = (D_MODEL, D_MODEL)
    w_query = (jax.random.normal(weight_keys[2], w_shape, jnp.float32) * fan_scale * head_q[None, :]).astype(jnp.bfloat16)
    w_key = (jax.random.normal(weight_keys[3], w_shape, jnp.float32) * fan_scale * head_k[None, :]).astype(jnp.bfloat16)
    w_value = (jax.random.normal(weight_keys[4], w_shape, jnp.float32) * fan_scale).astype(jnp.bfloat16)
    w_out = (jax.random.normal(weight_keys[5], w_shape, jnp.float32) * fan_scale).astype(jnp.bfloat16)
    g_norm = (1.0 + 0.3 * jax.random.normal(weight_keys[6], (D_MODEL,), jnp.float32)).astype(jnp.bfloat16)
    g_query = (1.7 + 0.4 * jax.random.normal(weight_keys[7], (D_MODEL,), jnp.float32)).astype(jnp.bfloat16)
    g_key = (1.7 + 0.4 * jax.random.normal(weight_keys[8], (D_MODEL,), jnp.float32)).astype(jnp.bfloat16)
    return {'x_in': x_in, 'grad_y': grad_y, 'positions': positions, 'g_norm': g_norm, 'w_query': w_query, 'w_key': w_key, 'w_value': w_value, 'w_out': w_out, 'g_query': g_query, 'g_key': g_key}


def rms_scale(values, gain_vec):
    inv_rms = lax.rsqrt(jnp.mean(values * values, axis=-1, keepdims=True) + NORM_EPS)
    return values * inv_rms * gain_vec


def rope_tables(positions):
    half_dim = HEAD_DIM // 2
    inv_freq = ROPE_BASE ** (-jnp.arange(half_dim, dtype=jnp.float32) * (2.0 / HEAD_DIM))
    angles = positions.astype(jnp.float32)[..., None] * inv_freq
    return jnp.cos(angles)[:, :, None, :], jnp.sin(angles)[:, :, None, :]


def rope_apply(values, cos_t, sin_t):
    half_dim = values.shape[-1] // 2
    first_half = values[..., :half_dim]
    second_half = values[..., half_dim:]
    return jnp.concatenate([first_half * cos_t - second_half * sin_t, second_half * cos_t + first_half * sin_t], axis=-1)


def mat_f32(left_op, right_op):
    return jnp.dot(left_op, right_op, precision=lax.Precision.HIGHEST)


def causal_attention(q_bf, k_bf, v_bf):
    q_f = q_bf.astype(jnp.float32)
    k_f = k_bf.astype(jnp.float32)
    v_f = v_bf.astype(jnp.float32)
    key_pos = jnp.arange(SEQ_LEN)
    qk_scale = HEAD_DIM ** -0.5

    def one_block(q_start):
        q_blk = lax.dynamic_slice_in_dim(q_f, q_start, QUERY_BLOCK, axis=1)
        scores = jnp.einsum('bqhd,bkhd->bhqk', q_blk, k_f, precision=lax.Precision.HIGHEST) * qk_scale
        q_pos = q_start + jnp.arange(QUERY_BLOCK)
        scores = jnp.where(q_pos[:, None] >= key_pos[None, :], scores, NEG_BIG)
        prob_f = jax.nn.softmax(scores, axis=-1)
        return jnp.einsum('bhqk,bkhd->bqhd', prob_f, v_f, precision=lax.Precision.HIGHEST)

    starts = jnp.arange(SEQ_LEN // QUERY_BLOCK) * QUERY_BLOCK
    blocks = lax.map(jax.checkpoint(one_block), starts)
    merged = jnp.moveaxis(blocks, 0, 1).reshape(q_bf.shape)
    return merged.astype(jnp.bfloat16)


def reference(x_in, grad_y, positions, g_norm, w_query, w_key, w_value, w_out, g_query, g_key):
    cos_t, sin_t = rope_tables(positions)
    head_shape = (N_BATCH, SEQ_LEN, N_HEADS, HEAD_DIM)
    flat_shape = (N_BATCH, SEQ_LEN, D_MODEL)

    def forward(x_f, gain_n, wq_f, wk_f, wv_f, wo_f, gain_q, gain_k):
        hidden = rms_scale(x_f, gain_n).astype(jnp.bfloat16).astype(jnp.float32)
        q_raw = mat_f32(hidden, wq_f)
        k_raw = mat_f32(hidden, wk_f)
        v_val = mat_f32(hidden, wv_f).astype(jnp.bfloat16)
        q_rot = rope_apply(rms_scale(q_raw, gain_q).reshape(head_shape), cos_t, sin_t).astype(jnp.bfloat16)
        k_rot = rope_apply(rms_scale(k_raw, gain_k).reshape(head_shape), cos_t, sin_t).astype(jnp.bfloat16)
        attended = causal_attention(q_rot, k_rot, v_val.reshape(head_shape))
        o_proj = mat_f32(attended.reshape(flat_shape).astype(jnp.float32), wo_f)
        return (x_f + o_proj).astype(jnp.bfloat16)

    y_out, pullback = jax.vjp(forward, x_in.astype(jnp.float32), g_norm.astype(jnp.float32), w_query.astype(jnp.float32), w_key.astype(jnp.float32), w_value.astype(jnp.float32), w_out.astype(jnp.float32), g_query.astype(jnp.float32), g_key.astype(jnp.float32))
    cotangents = pullback(grad_y)
    return (y_out, cotangents[0].astype(jnp.bfloat16), cotangents[1], cotangents[2], cotangents[3], cotangents[4], cotangents[5], cotangents[6], cotangents[7])
```

```python
import functools
import jax
import jax.numpy as jnp
from jax import lax
from jax.experimental import pallas as pl
from jax.experimental.pallas import tpu as pltpu
from jax.sharding import PartitionSpec as P

HEAD_DIM = 128
NORM_EPS = 1e-5
ROPE_BASE = 10000.0
NEG_BIG = -1e30
Q_BLK = 256
LOG2E = 1.4426950408889634


def mm(lhs, rhs):
    return lax.dot_general(lhs, rhs, (((1,), (0,)), ((), ())), preferred_element_type=jnp.float32)


def mm_nt(lhs, rhs):
    return lax.dot_general(lhs, rhs, (((1,), (1,)), ((), ())), preferred_element_type=jnp.float32)


def mm_tn(lhs, rhs):
    return lax.dot_general(lhs, rhs, (((0,), (0,)), ((), ())), preferred_element_type=jnp.float32)


def rope_tables(positions):
    half_dim = HEAD_DIM // 2
    inv_freq = ROPE_BASE ** (-jnp.arange(half_dim, dtype=jnp.float32) * (2.0 / HEAD_DIM))
    angles = positions.astype(jnp.float32)[..., None] * inv_freq
    cos_h, sin_h = jnp.cos(angles), jnp.sin(angles)
    return jnp.concatenate([cos_h, cos_h], axis=-1), jnp.concatenate([-sin_h, sin_h], axis=-1)


def rotate(values, cos_t, sin_t):
    return values * cos_t + pltpu.roll(values, HEAD_DIM // 2, 1) * sin_t


ANY_SPEC = pl.BlockSpec(memory_space=pltpu.HBM)
N_BLK = 256
MIB = 1024 * 1024
VMEM_MIB = 63


def bf_shape(*dims):
    return jax.ShapeDtypeStruct(dims, jnp.bfloat16)


def f32_shape(*dims):
    return jax.ShapeDtypeStruct(dims, jnp.float32)


def cost(flops, bytes_moved, exps=0):
    return pl.CostEstimate(flops=flops, bytes_accessed=bytes_moved, transcendentals=exps)


def limit(mib):
    return pltpu.CompilerParams(vmem_limit_bytes=max(mib, VMEM_MIB) * MIB)


def fixed(*dims):
    return pl.BlockSpec(dims, lambda i: (0,) * len(dims), pipeline_mode=pl.Buffered(1))


def qkv_kernel(x_ref, gain_ref, wq_ref, wk_ref, wv_ref, hid_ref, q_ref, k_ref, v_ref, qinv_ref, kinv_ref, qsum, ksum):
    step = pl.program_id(0)
    rows, width = x_ref.shape

    @pl.when(step == 0)
    def _():
        @pl.loop(0, rows // 128)
        def _(blk):
            span = pl.ds(pl.multiple_of(blk * 128, 128), 128)
            x_f = x_ref[span, :].astype(jnp.float32)
            inv_rms = lax.rsqrt(jnp.mean(x_f * x_f, axis=-1, keepdims=True) + NORM_EPS)
            hid_ref[span, :] = (x_f * inv_rms * gain_ref[...].astype(jnp.float32)).astype(jnp.bfloat16)

        qsum[...] = jnp.zeros_like(qsum)
        ksum[...] = jnp.zeros_like(ksum)

    for w_ref, out_ref, acc in ((wq_ref, q_ref, qsum), (wk_ref, k_ref, ksum)):
        raw = mm(hid_ref[...], w_ref[...])
        out_ref[...] = raw
        for part in range(N_BLK // 128):
            piece = raw[:, part * 128:(part + 1) * 128]
            acc[...] += piece * piece
    v_ref[...] = mm(hid_ref[...], wv_ref[...]).astype(jnp.bfloat16)

    @pl.when(step == pl.num_programs(0) - 1)
    def _():
        for acc, inv_ref in ((qsum, qinv_ref), (ksum, kinv_ref)):
            inv_ref[...] = lax.rsqrt(jnp.sum(acc[...], axis=-1, keepdims=True) * (1.0 / width) + NORM_EPS)


def qkv_call(x_seq, gain, w_query, w_key, w_value):
    rows, width = x_seq.shape
    w_col = pl.BlockSpec((width, N_BLK), lambda i: (0, i))
    o_col = pl.BlockSpec((rows, N_BLK), lambda i: (0, i))
    return pl.pallas_call(
        qkv_kernel, grid=(width // N_BLK,),
        in_specs=[fixed(rows, width), fixed(1, width), w_col, w_col, w_col],
        out_specs=[pl.BlockSpec((rows, width), lambda i: (0, 0)), o_col, o_col, o_col] + [pl.BlockSpec((rows, 1), lambda i: (0, 0))] * 2,
        out_shape=[bf_shape(rows, width), f32_shape(rows, width), f32_shape(rows, width), bf_shape(rows, width), f32_shape(rows, 1), f32_shape(rows, 1)],
        scratch_shapes=[pltpu.VMEM((rows, 128), jnp.float32)] * 2,
        cost_estimate=cost(6 * rows * width * width, 6 * width * width + 14 * rows * width),
        compiler_params=limit(48), name="qkv",
    )(x_seq, gain.reshape(1, width), w_query, w_key, w_value)


def rope_heads(q1_ref, k1_ref, qinv_ref, kinv_ref, gq_ref, gk_ref, cos_ref, sin_ref, q_s, k_s):
    cos_t, sin_t = cos_ref[...], sin_ref[...]
    q_s[...] = rotate(q1_ref[...] * qinv_ref[...] * gq_ref[...].astype(jnp.float32), cos_t, sin_t).astype(jnp.bfloat16)
    k_s[...] = rotate(k1_ref[...] * kinv_ref[...] * gk_ref[...].astype(jnp.float32), cos_t, sin_t).astype(jnp.bfloat16)


def masked_scores(keys, q_blk, q_lo):
    scores = mm_nt(keys, q_blk)
    edge = scores[q_lo:, :]
    key_pos = lax.broadcasted_iota(jnp.int32, edge.shape, 0)
    q_pos = lax.broadcasted_iota(jnp.int32, edge.shape, 1)
    edge = jnp.where(q_pos >= key_pos, edge, NEG_BIG)
    return edge if q_lo == 0 else jnp.concatenate([scores[:q_lo, :], edge], axis=0)


def attn_fwd_kernel(q1_ref, k1_ref, v_ref, qinv_ref, kinv_ref, gq_ref, gk_ref, cos_ref, sin_ref, a_ref, q_s, k_s, lse_ref):
    seq = q1_ref.shape[0]
    rope_heads(q1_ref, k1_ref, qinv_ref, kinv_ref, gq_ref, gk_ref, cos_ref, sin_ref, q_s, k_s)
    to_log2 = HEAD_DIM ** -0.5 * LOG2E
    v_t = v_ref[...].T
    for blk in range(seq // Q_BLK):
        q_lo, k_len = blk * Q_BLK, (blk + 1) * Q_BLK
        scores = masked_scores(k_s[:k_len, :], q_s[q_lo:k_len, :], q_lo)
        top = jnp.max(scores, axis=0, keepdims=True)
        prob = jnp.exp2((scores - top) * to_log2)
        total = jnp.sum(prob, axis=0, keepdims=True)
        out_t = mm(v_t[:, :k_len], prob.astype(jnp.bfloat16)) * (1.0 / total)
        a_ref[q_lo:k_len, :] = out_t.T.astype(jnp.bfloat16)
        lse_ref[0, :, q_lo:k_len] = top * to_log2 + jnp.log2(total)


def attn_bwd_kernel(q_ref, k_ref, v_ref, do_ref, lse_ref, dep_ref, dq_ref, dk_ref, dv_ref, dk_s, dv_s):
    seq = q_ref.shape[0]
    scale = HEAD_DIM ** -0.5
    k_t = k_ref[...].T
    n_blk = seq // Q_BLK
    for blk in reversed(range(n_blk)):
        q_lo, k_len = blk * Q_BLK, (blk + 1) * Q_BLK
        q_blk = q_ref[q_lo:k_len, :]
        do_blk = do_ref[q_lo:k_len, :]
        scores = masked_scores(k_ref[:k_len, :], q_blk, q_lo)
        prob = jnp.exp2(scores * (scale * LOG2E) - lse_ref[0, :, q_lo:k_len])
        d_prob = mm_nt(v_ref[:k_len, :], do_blk)
        row_dot = jnp.sum(prob * d_prob, axis=0, keepdims=True)
        ds_bf = (prob * ((d_prob - row_dot) * scale)).astype(jnp.bfloat16)
        dq_t = mm(k_t[:, :k_len], ds_bf)
        dq_ref[q_lo:k_len, :] = dq_t.T.astype(jnp.bfloat16)
        dv_part = mm(prob.astype(jnp.bfloat16), do_blk)
        dk_part = mm(ds_bf, q_blk)
        if blk == n_blk - 1:
            dv_s[...] = dv_part
            dk_s[...] = dk_part
        else:
            dv_s[:k_len, :] += dv_part
            dk_s[:k_len, :] += dk_part
    dv_ref[...] = dv_s[...].astype(jnp.bfloat16)
    dk_ref[...] = dk_s[...].astype(jnp.bfloat16)


def attn_specs(seq):
    head = pl.BlockSpec((seq, HEAD_DIM), lambda h: (0, h))
    lse = pl.BlockSpec((1, 1, seq), lambda h: (h, 0, 0))
    return head, lse


def attn_fwd_call(q_raw, k_raw, v_val, q_inv, k_inv, g_query, g_key, cos_t, sin_t):
    seq, width = q_raw.shape
    n_heads = width // HEAD_DIM
    head, lse = attn_specs(seq)
    gain = pl.BlockSpec((1, HEAD_DIM), lambda h: (0, h))
    return pl.pallas_call(
        attn_fwd_kernel, grid=(n_heads,),
        in_specs=[head, head, head, fixed(seq, 1), fixed(seq, 1), gain, gain, fixed(seq, HEAD_DIM), fixed(seq, HEAD_DIM)],
        out_specs=[head, head, head, lse],
        out_shape=[bf_shape(seq, width)] * 3 + [f32_shape(n_heads, 1, seq)],
        cost_estimate=cost(4 * seq * seq * width, 16 * seq * width, seq * seq * n_heads // 2),
        compiler_params=limit(40), name="attention_fwd",
    )(q_raw, k_raw, v_val, q_inv, k_inv, g_query.reshape(1, width), g_key.reshape(1, width), cos_t, sin_t)


def attn_bwd_call(q_bf, k_bf, v_val, d_attn, lse_all, dep):
    seq, width = q_bf.shape
    n_heads = width // HEAD_DIM
    head, lse = attn_specs(seq)
    return pl.pallas_call(
        attn_bwd_kernel, grid=(n_heads,),
        in_specs=[head, head, head, head, lse, ANY_SPEC],
        out_specs=[head] * 3, out_shape=[bf_shape(seq, width)] * 3,
        scratch_shapes=[pltpu.VMEM((seq, HEAD_DIM), jnp.float32)] * 2,
        cost_estimate=cost(10 * seq * seq * width, 14 * seq * width, seq * seq * n_heads // 2),
        compiler_params=limit(40), name="attention_bwd",
    )(q_bf, k_bf, v_val, d_attn, lse_all, dep)


def out_kernel(a_ref, w_ref, x_ref, dep_ref, y_ref):
    y_ref[...] = (x_ref[...].astype(jnp.float32) + mm(a_ref[...], w_ref[...])).astype(jnp.bfloat16)


def out_call(attended, w_out, x_seq, dep):
    rows, width = x_seq.shape
    o_col = pl.BlockSpec((rows, N_BLK), lambda i: (0, i))
    return pl.pallas_call(
        out_kernel, grid=(width // N_BLK,),
        in_specs=[fixed(rows, width), pl.BlockSpec((width, N_BLK), lambda i: (0, i)), o_col, ANY_SPEC],
        out_specs=o_col, out_shape=bf_shape(rows, width),
        cost_estimate=cost(2 * rows * width * width, 2 * width * width + 6 * rows * width),
        compiler_params=limit(32), name="project_out",
    )(attended, w_out, x_seq, dep)


def head_grad_kernel(gy_ref, w_ref, dep_ref, out_ref):
    out_ref[...] = mm_nt(gy_ref[...], w_ref[...]).astype(jnp.bfloat16)


def head_grad_call(gy_seq, w_out, dep):
    rows, width = gy_seq.shape
    return pl.pallas_call(
        head_grad_kernel, grid=(width // N_BLK,),
        in_specs=[fixed(rows, width), pl.BlockSpec((N_BLK, width), lambda i: (i, 0)), ANY_SPEC],
        out_specs=pl.BlockSpec((rows, N_BLK), lambda i: (0, i)), out_shape=bf_shape(rows, width),
        cost_estimate=cost(2 * rows * width * width, 2 * width * width + 4 * rows * width),
        compiler_params=limit(32), name="head_grad",
    )(gy_seq, w_out, dep)


def copy_kernel(in_ref, dep_ref, out_ref):
    out_ref[...] = in_ref[...]


def copy_call(values, dep):
    blk = pl.BlockSpec((1,) + values.shape[1:], lambda i: (i, 0, 0))
    return pl.pallas_call(
        copy_kernel, grid=(values.shape[0],), in_specs=[blk, ANY_SPEC], out_specs=blk,
        out_shape=jax.ShapeDtypeStruct(values.shape, values.dtype),
        cost_estimate=cost(0, 4 * values.size), compiler_params=limit(16), name="store_rows",
    )(values, dep)


def hid_grad_kernel(dq_ref, dk_ref, dv_ref, wq_ref, wk_ref, wv_ref, dep_ref, out_ref):
    out_ref[...] = mm_nt(dq_ref[...], wq_ref[...]) + mm_nt(dk_ref[...], wk_ref[...]) + mm_nt(dv_ref[...], wv_ref[...])


def hid_grad_call(dq_raw, dk_raw, dv_bf, w_query, w_key, w_value, dep):
    rows, width = dq_raw.shape
    w_row = pl.BlockSpec((N_BLK, width), lambda i: (i, 0))
    return pl.pallas_call(
        hid_grad_kernel, grid=(width // N_BLK,),
        in_specs=[fixed(rows, width)] * 3 + [w_row] * 3 + [ANY_SPEC],
        out_specs=pl.BlockSpec((rows, N_BLK), lambda i: (0, i)), out_shape=f32_shape(rows, width),
        cost_estimate=cost(6 * rows * width * width, 6 * width * width + 10 * rows * width),
        compiler_params=limit(40), name="hidden_grad",
    )(dq_raw, dk_raw, dv_bf, w_query, w_key, w_value, dep)


def x_grad_kernel(dh_ref, x_ref, gy_ref, gain_ref, gx_ref, gsum_ref):
    x_f = x_ref[...].astype(jnp.float32)
    inv_rms = lax.rsqrt(jnp.mean(x_f * x_f, axis=-1, keepdims=True) + NORM_EPS)
    hat = x_f * inv_rms
    d_hid = dh_ref[...]

    @pl.when(pl.program_id(0) == 0)
    def _():
        gsum_ref[...] = jnp.zeros_like(gsum_ref)

    gsum_ref[...] += jnp.sum(d_hid * hat, axis=0, keepdims=True)
    d_nrm = d_hid * gain_ref[...].astype(jnp.float32)
    d_x = inv_rms * (d_nrm - hat * jnp.mean(d_nrm * hat, axis=-1, keepdims=True))
    gx_ref[...] = (gy_ref[...].astype(jnp.float32) + d_x).astype(jnp.bfloat16)


def x_grad_call(d_hid, x_seq, gy_seq, gain):
    rows, width = x_seq.shape
    row_blk = pl.BlockSpec((128, width), lambda i: (i, 0))
    vec = pl.BlockSpec((1, width), lambda i: (0, 0))
    return pl.pallas_call(
        x_grad_kernel, grid=(rows // 128,),
        in_specs=[row_blk, row_blk, row_blk, vec], out_specs=[row_blk, vec],
        out_shape=[bf_shape(rows, width), f32_shape(1, width)],
        cost_estimate=cost(12 * rows * width, 10 * rows * width), compiler_params=limit(16), name="input_grad",
    )(d_hid, x_seq, gy_seq, gain.reshape(1, width))


def weight_kernel(idx_ref, la_ref, lb_ref, ra_ref, rb_ref, dep_ref, xl_ref, yr_ref, kl_ref, kr_ref):
    step = pl.program_id(0)
    y_bit, x_bit = step // 2, lax.rem(step, 2)
    half = kl_ref.shape[-1]
    for lo, (near, far, pick, slot) in ((0, (kl_ref, xl_ref, x_bit, y_bit)), (half, (kr_ref, yr_ref, y_bit, x_bit))):
        part = mm_tn(la_ref[...], ra_ref[:, lo:lo + half]) + mm_tn(lb_ref[...], rb_ref[:, lo:lo + half])

        @pl.when(pick == 0)
        def _():
            near[pl.ds(slot, 1)] = part[None]

        @pl.when(pick == 1)
        def _():
            far[pl.ds(slot, 1)] = part[None]


def weight_call(idx, left_mine, left_peer, right_mine, right_peer, dep):
    rows, width = left_mine.shape
    blk = width // 8
    left = pl.BlockSpec((rows, blk), lambda i, idx_ref: (0, idx_ref[i]))
    right = pl.BlockSpec((rows, width), lambda i, idx_ref: (0, 0), pipeline_mode=pl.Buffered(1))
    out = pl.BlockSpec((2, blk, width // 2), lambda i, idx_ref: (0, 0, 0))
    return pl.pallas_call(
        weight_kernel,
        grid_spec=pltpu.PrefetchScalarGridSpec(
            num_scalar_prefetch=1, grid=(4,),
            in_specs=[left, left, right, right, ANY_SPEC], out_specs=[out] * 4),
        out_shape=[f32_shape(2, blk, width // 2)] * 4,
        cost_estimate=cost(4 * rows * width * width // 2, 12 * rows * width + 2 * width * width),
        compiler_params=limit(48), name="weight_grad",
    )(idx, left_mine, left_peer, right_mine, right_peer, dep)


def merge_kernel(kl_ref, rl_ref, kr_ref, rr_ref, dep_ref, stay_l, away_l, stay_r, away_r):
    stay_l[...] = kl_ref[0] + rl_ref[0]
    away_l[...] = kl_ref[1] + rl_ref[1]
    stay_r[...] = kr_ref[0] + rr_ref[0]
    away_r[...] = kr_ref[1] + rr_ref[1]


def merge_call(keep_l, recv_l, keep_r, recv_r, dep):
    _, rows, cols = keep_l.shape
    inp = pl.BlockSpec((2, 64, cols), lambda i: (0, i, 0))
    out = pl.BlockSpec((64, cols), lambda i: (i, 0))
    return pl.pallas_call(
        merge_kernel, grid=(rows // 64,), in_specs=[inp] * 4 + [ANY_SPEC], out_specs=[out] * 4,
        out_shape=[f32_shape(rows, cols)] * 4,
        cost_estimate=cost(4 * rows * cols, 48 * rows * cols), compiler_params=limit(16), name="merge",
    )(keep_l, recv_l, keep_r, recv_r, dep)


def final_kernel(sl_ref, rl_ref, sr_ref, rr_ref, dep_ref, out_ref):
    half = sl_ref.shape[-1]
    out_ref[:, :half] = sl_ref[...] + rl_ref[...]
    out_ref[:, half:] = sr_ref[...] + rr_ref[...]


def final_call(stay_l, recv_l, stay_r, recv_r, dep):
    rows, cols = stay_l.shape
    inp = pl.BlockSpec((64, cols), lambda i: (i, 0))
    return pl.pallas_call(
        final_kernel, grid=(rows // 64,), in_specs=[inp] * 4 + [ANY_SPEC],
        out_specs=pl.BlockSpec((64, 2 * cols), lambda i: (i, 0)), out_shape=f32_shape(rows, 2 * cols),
        cost_estimate=cost(2 * rows * cols, 24 * rows * cols), compiler_params=limit(16), name="final_add",
    )(stay_l, recv_l, stay_r, recv_r, dep)


def unnorm_kernel(dq_ref, raw_ref, inv_ref, gain_ref, cos_ref, sin_ref, dep_ref, out_ref, gsum_ref, dn_s, hat_s):
    blk, width = raw_ref.shape
    cos_t, sin_t = cos_ref[...], -sin_ref[...]
    inv_rms = inv_ref[...]

    @pl.when(pl.program_id(0) == 0)
    def _():
        gsum_ref[...] = jnp.zeros_like(gsum_ref)

    acc = jnp.zeros((blk, HEAD_DIM), jnp.float32)
    for head in range(width // HEAD_DIM):
        cols = slice(head * HEAD_DIM, (head + 1) * HEAD_DIM)
        d_out = rotate(dq_ref[:, cols].astype(jnp.float32), cos_t, sin_t)
        hat = raw_ref[:, cols] * inv_rms
        gsum_ref[:, cols] += jnp.sum(d_out * hat, axis=0, keepdims=True)
        d_nrm = d_out * gain_ref[:, cols].astype(jnp.float32)
        acc += d_nrm * hat
        dn_s[:, cols] = d_nrm
        hat_s[:, cols] = hat
    mean = jnp.sum(acc, axis=-1, keepdims=True) * (1.0 / width)
    out_ref[...] = (inv_rms * (dn_s[...] - hat_s[...] * mean)).astype(jnp.bfloat16)


def unnorm_call(d_rot, raw, inv_rms, gain, cos_t, sin_t, dep):
    rows, width = raw.shape
    blk = 128
    row_blk = pl.BlockSpec((blk, width), lambda i: (i, 0))
    vec = pl.BlockSpec((1, width), lambda i: (0, 0))
    tab = pl.BlockSpec((blk, HEAD_DIM), lambda i: (i, 0))
    return pl.pallas_call(
        unnorm_kernel, grid=(rows // blk,),
        in_specs=[row_blk, row_blk, pl.BlockSpec((blk, 1), lambda i: (i, 0)), vec, tab, tab, ANY_SPEC],
        out_specs=[row_blk, vec],
        out_shape=[jax.ShapeDtypeStruct((rows, width), jnp.bfloat16), jax.ShapeDtypeStruct((1, width), jnp.float32)],
        scratch_shapes=[pltpu.VMEM((blk, width), jnp.float32)] * 2,
        cost_estimate=pl.CostEstimate(flops=rows * width * 12, bytes_accessed=rows * width * 8, transcendentals=0),
        compiler_params=limit(16), name="unnorm",
    )(d_rot, raw, inv_rms, gain.reshape(1, width), cos_t, sin_t, dep)


def solution(mesh):
    n_sp = mesh.shape['sp']
    swap = functools.partial(lax.all_to_all, axis_name='sp', split_axis=0, concat_axis=0, tiled=True)

    def flip(values, bit):
        return lax.ppermute(values, 'sp', [(dev, dev ^ bit) for dev in range(n_sp)])

    def block_step(x_loc, grad_y, positions, g_norm, w_query, w_key, w_value, w_out, g_query, g_key):
        n_batch, loc_len, width = x_loc.shape
        seq = n_sp * loc_len
        rows = width // n_sp
        me = lax.axis_index('sp')
        idx = me ^ jnp.array([0, 2, 4, 6], jnp.int32)

        def first_hop(parts):
            far_l, far_r, near_l, near_r = parts
            return near_l, flip(far_l, 2), near_r, flip(far_r, 4)

        def second_hop(parts):
            stay_l, away_l, stay_r, away_r = parts
            return stay_l, flip(away_l, 4), stay_r, flip(away_r, 2)

        cos_t, sin_t = rope_tables(swap(positions).reshape(seq))
        x_seq = swap(x_loc).reshape(seq, width)
        gy_seq = swap(grad_y).reshape(seq, width)
        hidden, q_raw, k_raw, v_val, q_inv, k_inv = qkv_call(x_seq, g_norm, w_query, w_key, w_value)
        attended, q_bf, k_bf, lse_all = attn_fwd_call(q_raw, k_raw, v_val, q_inv, k_inv, g_query, g_key, cos_t, sin_t)
        a_peer = flip(attended, 1)
        gy_peer = flip(gy_seq, 1)
        hid_peer = flip(hidden, 1)
        y_seq = out_call(attended, w_out, x_seq, attended)
        y_swap = swap(y_seq.reshape(n_batch, loc_len, width))
        part_o = weight_call(idx, attended, a_peer, gy_seq, gy_peer, y_seq)
        hop_o = first_hop(part_o)
        d_attn = head_grad_call(gy_seq, w_out, part_o[2])
        dq_bf, dk_bf, dv_bf = attn_bwd_call(q_bf, k_bf, v_val, d_attn, lse_all, y_seq)
        dv_peer = flip(dv_bf, 1)
        mrg_o = merge_call(*hop_o, dv_bf)
        fin_o = second_hop(mrg_o)
        part_v = weight_call(idx, hidden, hid_peer, dv_bf, dv_peer, mrg_o[0])
        hop_v = first_hop(part_v)
        dq_raw, gq_sum = unnorm_call(dq_bf, q_raw, q_inv, g_query, cos_t, sin_t, part_v[2])
        dq_peer = flip(dq_raw, 1)
        dk_raw, gk_sum = unnorm_call(dk_bf, k_raw, k_inv, g_key, cos_t, sin_t, dq_raw)
        dk_peer = flip(dk_raw, 1)
        part_q = weight_call(idx, hidden, hid_peer, dq_raw, dq_peer, dk_raw)
        hop_q = first_hop(part_q)
        part_k = weight_call(idx, hidden, hid_peer, dk_raw, dk_peer, part_q[2])
        hop_k = first_hop(part_k)
        d_hid = hid_grad_call(dq_raw, dk_raw, dv_bf, w_query, w_key, w_value, part_k[2])
        gx_seq, gn_sum = x_grad_call(d_hid, x_seq, gy_seq, g_norm)
        gx_swap = swap(gx_seq.reshape(n_batch, loc_len, width))
        gains = jnp.concatenate([gn_sum, gq_sum, gk_sum], axis=0)
        cut = [lax.dynamic_slice_in_dim(gains, (me ^ off) * rows, rows, axis=1) for off in range(n_sp)]
        gain_rows = sum((flip(cut[off], off) for off in range(1, n_sp)), cut[0])
        mrg_v = merge_call(*hop_v, gx_seq)
        fin_v = second_hop(mrg_v)
        mrg_q = merge_call(*hop_q, mrg_v[0])
        fin_q = second_hop(mrg_q)
        y_out = copy_call(y_swap, mrg_q[0])
        mrg_k = merge_call(*hop_k, y_out)
        fin_k = second_hop(mrg_k)
        grad_wo = final_call(*fin_o, mrg_k[0])
        grad_x = copy_call(gx_swap, grad_wo)
        grad_wv = final_call(*fin_v, grad_x)
        grad_wq = final_call(*fin_q, grad_wv)
        grad_wk = final_call(*fin_k, grad_wq)
        return (y_out, grad_x, gain_rows[0], grad_wq, grad_wk, grad_wv, grad_wo, gain_rows[1], gain_rows[2])

    seq_spec = P('dp', 'sp', None)
    mat_rep = P(None, None)
    vec_rep = P(None)
    row_spec = P(('dp', 'sp'), None)
    vec_spec = P(('dp', 'sp'))
    return jax.shard_map(block_step, mesh=mesh, in_specs=(seq_spec, seq_spec, P('dp', 'sp'), vec_rep, mat_rep, mat_rep, mat_rep, mat_rep, vec_rep, vec_rep), out_specs=(seq_spec, seq_spec, vec_spec, row_spec, row_spec, row_spec, row_spec, vec_spec, vec_spec), check_vma=False)
```

```python
import functools
import jax
import jax.numpy as jnp
from jax import lax
from jax.experimental import pallas as pl
from jax.experimental.pallas import tpu as pltpu
from jax.sharding import PartitionSpec as P

HEAD_DIM = 128
NORM_EPS = 1e-5
ROPE_BASE = 10000.0
NEG_BIG = -1e30
Q_BLK = 256
LOG2E = 1.4426950408889634


def mm(lhs, rhs):
    return lax.dot_general(lhs, rhs, (((1,), (0,)), ((), ())), preferred_element_type=jnp.float32)


def mm_nt(lhs, rhs):
    return lax.dot_general(lhs, rhs, (((1,), (1,)), ((), ())), preferred_element_type=jnp.float32)


def mm_tn(lhs, rhs):
    return lax.dot_general(lhs, rhs, (((0,), (0,)), ((), ())), preferred_element_type=jnp.float32)


def rope_tables(positions):
    half_dim = HEAD_DIM // 2
    inv_freq = ROPE_BASE ** (-jnp.arange(half_dim, dtype=jnp.float32) * (2.0 / HEAD_DIM))
    angles = positions.astype(jnp.float32)[..., None] * inv_freq
    cos_h, sin_h = jnp.cos(angles), jnp.sin(angles)
    return jnp.concatenate([cos_h, cos_h], axis=-1), jnp.concatenate([-sin_h, sin_h], axis=-1)


def rotate(values, cos_t, sin_t):
    return values * cos_t + pltpu.roll(values, HEAD_DIM // 2, 1) * sin_t


ANY_SPEC = pl.BlockSpec(memory_space=pltpu.HBM)
N_BLK = 256
MIB = 1024 * 1024
VMEM_MIB = 63
HEADS = 2
WIDE = 512


def bf_shape(*dims):
    return jax.ShapeDtypeStruct(dims, jnp.bfloat16)


def f32_shape(*dims):
    return jax.ShapeDtypeStruct(dims, jnp.float32)


def cost(flops, bytes_moved, exps=0):
    return pl.CostEstimate(flops=flops, bytes_accessed=bytes_moved, transcendentals=exps)


def limit(mib):
    return pltpu.CompilerParams(vmem_limit_bytes=max(mib, VMEM_MIB) * MIB)


def fixed(*dims):
    return pl.BlockSpec(dims, lambda i: (0,) * len(dims), pipeline_mode=pl.Buffered(1))


def partner_of(me, off):
    flipped = me
    for bit in (1, 2, 4):
        if off & bit:
            flipped = flipped + bit - 2 * bit * ((me // bit) % 2)
    return flipped


def gather_qkv_kernel(x_ref, pos_ref, gain_ref, wq_ref, wk_ref, wv_ref, xs_ref, hid_ref, q_ref, k_ref, v_ref, qinv_ref, kinv_ref, pos_out,
                      x_s, pos_s, wq_s, wk_s, wv_s, hid_s, q_s, k_s, v_s, send_sem, recv_sem, psend_sem, precv_sem, w_sem, own_sem, x_out_sem, out_sem):
    n_sp, tok, width = x_ref.shape
    me = lax.axis_index('sp')
    pair = 2 * tok
    barrier = pltpu.get_barrier_semaphore()
    for off in range(1, n_sp):
        pl.semaphore_signal(barrier, inc=1, device_id={'sp': partner_of(me, off)}, device_id_type=pl.DeviceIdType.MESH)
    pl.semaphore_wait(barrier, n_sp - 1)

    copies, pos_copies = [], []
    for off in range(n_sp):
        peer = partner_of(me, off)
        if off == 0:
            copies.append(pltpu.make_async_copy(x_ref.at[me], x_s.at[me], own_sem.at[0]))
            pos_copies.append(pltpu.make_async_copy(pos_ref.at[me], pos_s.at[me], own_sem.at[1]))
        else:
            pos_copies.append(pltpu.make_async_remote_copy(
                src_ref=pos_ref.at[peer], dst_ref=pos_s.at[me], send_sem=psend_sem.at[off], recv_sem=precv_sem.at[off],
                device_id={'sp': peer}, device_id_type=pl.DeviceIdType.MESH))
            copies.append(pltpu.make_async_remote_copy(
                src_ref=x_ref.at[peer], dst_ref=x_s.at[me], send_sem=send_sem.at[off], recv_sem=recv_sem.at[off],
                device_id={'sp': peer}, device_id_type=pl.DeviceIdType.MESH))
        pos_copies[-1].start()
        copies[-1].start()
    loads = [pltpu.make_async_copy(src, dst, w_sem.at[i]) for i, (src, dst) in enumerate(((wq_ref, wq_s), (wk_ref, wk_s), (wv_ref, wv_s)))]
    for load in loads:
        load.start()

    outs = []
    for step in range(n_sp // 2):
        slot = step % 2
        chip = partner_of(me, 2 * step) // 2
        if step == 0:
            copies[0].wait()
        else:
            copies[2 * step].wait_recv()
        copies[2 * step + 1].wait_recv()
        rows = pl.ds(pl.multiple_of(chip * pair, pair), pair)
        if step >= 2:
            for out in outs[step - 2]:
                out.wait()
        for part in range(2):
            x_f = x_s[2 * chip + part].astype(jnp.float32)
            inv_rms = lax.rsqrt(jnp.mean(x_f * x_f, axis=-1, keepdims=True) + NORM_EPS)
            hid_s[slot, part * tok:(part + 1) * tok, :] = (x_f * inv_rms * gain_ref[...].astype(jnp.float32)).astype(jnp.bfloat16)
        if step == 0:
            for load in loads:
                load.wait()

        def columns(blk, sums):
            cols = pl.ds(pl.multiple_of(blk * N_BLK, N_BLK), N_BLK)
            hid = hid_s[slot]
            new_sums = []
            for w_s, dst, total in ((wq_s, q_s, sums[0]), (wk_s, k_s, sums[1])):
                raw = mm(hid, w_s[:, cols])
                dst[slot, :, cols] = raw
                for lo in range(0, N_BLK, 128):
                    total = total + raw[:, lo:lo + 128] * raw[:, lo:lo + 128]
                new_sums.append(total)
            v_s[slot, :, cols] = mm(hid, wv_s[:, cols]).astype(jnp.bfloat16)
            return tuple(new_sums)

        zero = jnp.zeros((pair, 128), jnp.float32)
        sums = lax.fori_loop(0, width // N_BLK, columns, (zero, zero))
        for total, inv_ref in zip(sums, (qinv_ref, kinv_ref)):
            inv_ref[rows, :] = lax.rsqrt(jnp.sum(total, axis=-1, keepdims=True) * (1.0 / width) + NORM_EPS)
        group = [pltpu.make_async_copy(src.at[slot], dst.at[rows], out_sem.at[slot, i])
                 for i, (src, dst) in enumerate(((hid_s, hid_ref), (q_s, q_ref), (k_s, k_ref), (v_s, v_ref)))]
        for part in range(2):
            group.append(pltpu.make_async_copy(x_s.at[2 * chip + part], xs_ref.at[2 * chip + part], x_out_sem.at[2 * step + part]))
        for out in group:
            out.start()
        outs.append(group)
    for group in outs[-2:]:
        for out in group:
            out.wait()
    pos_copies[0].wait()
    for off in range(1, n_sp):
        pos_copies[off].wait()
        copies[off].wait_send()
    pos_out[...] = pos_s[...]


def gather_qkv_call(x_loc, positions, gain, w_query, w_key, w_value):
    n_sp, tok, width = x_loc.shape
    rows, pair = n_sp * tok, 2 * tok
    hbm = pl.BlockSpec(memory_space=pltpu.HBM)
    vmem = pl.BlockSpec(memory_space=pltpu.VMEM)
    dma = pltpu.SemaphoreType.DMA
    return pl.pallas_call(
        gather_qkv_kernel,
        in_specs=[hbm, hbm, vmem, hbm, hbm, hbm],
        out_specs=[hbm] * 5 + [vmem] * 3,
        out_shape=[bf_shape(n_sp, tok, width), bf_shape(rows, width), f32_shape(rows, width), f32_shape(rows, width), bf_shape(rows, width),
                   f32_shape(rows, 1), f32_shape(rows, 1), jax.ShapeDtypeStruct((n_sp, 1, tok), jnp.int32)],
        scratch_shapes=[
            pltpu.VMEM((n_sp, tok, width), jnp.bfloat16), pltpu.VMEM((n_sp, 1, tok), jnp.int32)]
        + [pltpu.VMEM((width, width), jnp.bfloat16)] * 3
        + [pltpu.VMEM((2, pair, width), jnp.bfloat16), pltpu.VMEM((2, pair, width), jnp.float32), pltpu.VMEM((2, pair, width), jnp.float32), pltpu.VMEM((2, pair, width), jnp.bfloat16)]
        + [dma((n_sp,)), dma((n_sp,)), dma((n_sp,)), dma((n_sp,)), dma((3,)), dma((2,)), dma((n_sp,)), dma((2, 4))],
        cost_estimate=cost(6 * rows * width * width, 6 * width * width + 14 * rows * width),
        compiler_params=pltpu.CompilerParams(vmem_limit_bytes=VMEM_MIB * MIB, collective_id=0, has_side_effects=True),
        name="gather_qkv",
    )(x_loc, positions.reshape(n_sp, 1, tok), gain.reshape(1, width), w_query, w_key, w_value)


def rope_heads(q1_ref, k1_ref, qinv_ref, kinv_ref, gq_ref, gk_ref, cos_ref, sin_ref, q_s, k_s, cols):
    cos_t, sin_t = cos_ref[...], sin_ref[...]
    q_s[:, cols] = rotate(q1_ref[:, cols] * qinv_ref[...] * gq_ref[:, cols].astype(jnp.float32), cos_t, sin_t).astype(jnp.bfloat16)
    k_s[:, cols] = rotate(k1_ref[:, cols] * kinv_ref[...] * gk_ref[:, cols].astype(jnp.float32), cos_t, sin_t).astype(jnp.bfloat16)


def masked_scores(keys, q_blk, q_lo):
    scores = mm_nt(keys, q_blk)
    edge = scores[q_lo:, :]
    key_pos = lax.broadcasted_iota(jnp.int32, edge.shape, 0)
    q_pos = lax.broadcasted_iota(jnp.int32, edge.shape, 1)
    edge = jnp.where(q_pos >= key_pos, edge, NEG_BIG)
    return edge if q_lo == 0 else jnp.concatenate([scores[:q_lo, :], edge], axis=0)


def head_cols(head):
    return slice(head * HEAD_DIM, (head + 1) * HEAD_DIM)


def attn_fwd_kernel(q1_ref, k1_ref, v_ref, qinv_ref, kinv_ref, gq_ref, gk_ref, cos_ref, sin_ref, a_ref, q_s, k_s, lse_ref):
    seq = q1_ref.shape[0]
    to_log2 = HEAD_DIM ** -0.5 * LOG2E
    for head in range(HEADS):
        rope_heads(q1_ref, k1_ref, qinv_ref, kinv_ref, gq_ref, gk_ref, cos_ref, sin_ref, q_s, k_s, head_cols(head))
    v_t = [v_ref[:, head_cols(head)].T for head in range(HEADS)]
    for blk in range(seq // Q_BLK):
        q_lo, k_len = blk * Q_BLK, (blk + 1) * Q_BLK
        scores = [masked_scores(k_s[:k_len, head_cols(h)], q_s[q_lo:k_len, head_cols(h)], q_lo) for h in range(HEADS)]
        for head in range(HEADS):
            top = jnp.max(scores[head], axis=0, keepdims=True)
            prob = jnp.exp2((scores[head] - top) * to_log2)
            total = jnp.sum(prob, axis=0, keepdims=True)
            out_t = mm(v_t[head][:, :k_len], prob.astype(jnp.bfloat16)) * (1.0 / total)
            a_ref[q_lo:k_len, head_cols(head)] = out_t.T.astype(jnp.bfloat16)
            lse_ref[head, :, q_lo:k_len] = top * to_log2 + jnp.log2(total)


def attn_bwd_kernel(q_ref, k_ref, v_ref, do_ref, lse_ref, dep_ref, dq_ref, dk_ref, dv_ref, dk_s, dv_s):
    seq = q_ref.shape[0]
    scale = HEAD_DIM ** -0.5
    k_t = [k_ref[:, head_cols(head)].T for head in range(1)]
    n_blk = seq // Q_BLK
    for blk in reversed(range(n_blk)):
        q_lo, k_len = blk * Q_BLK, (blk + 1) * Q_BLK
        for head in range(1):
            cols = head_cols(head)
            q_blk = q_ref[q_lo:k_len, cols]
            do_blk = do_ref[q_lo:k_len, cols]
            scores = masked_scores(k_ref[:k_len, cols], q_blk, q_lo)
            prob = jnp.exp2(scores * (scale * LOG2E) - lse_ref[head, :, q_lo:k_len])
            d_prob = mm_nt(v_ref[:k_len, cols], do_blk)
            row_dot = jnp.sum(prob * d_prob, axis=0, keepdims=True)
            ds_bf = (prob * ((d_prob - row_dot) * scale)).astype(jnp.bfloat16)
            dq_t = mm(k_t[head][:, :k_len], ds_bf)
            dq_ref[q_lo:k_len, cols] = dq_t.T.astype(jnp.bfloat16)
            dv_part = mm(prob.astype(jnp.bfloat16), do_blk)
            dk_part = mm(ds_bf, q_blk)
            if blk == n_blk - 1:
                dv_s[:, cols] = dv_part
                dk_s[:, cols] = dk_part
            else:
                dv_s[:k_len, cols] += dv_part
                dk_s[:k_len, cols] += dk_part
    dv_ref[...] = dv_s[...].astype(jnp.bfloat16)
    dk_ref[...] = dk_s[...].astype(jnp.bfloat16)


def attn_specs(seq, heads):
    head = pl.BlockSpec((seq, heads * HEAD_DIM), lambda h: (0, h))
    lse = pl.BlockSpec((heads, 1, seq), lambda h: (h, 0, 0))
    return head, lse


def attn_fwd_call(q_raw, k_raw, v_val, q_inv, k_inv, g_query, g_key, cos_t, sin_t):
    seq, width = q_raw.shape
    n_heads = width // HEAD_DIM
    head, lse = attn_specs(seq, HEADS)
    gain = pl.BlockSpec((1, HEADS * HEAD_DIM), lambda h: (0, h))
    return pl.pallas_call(
        attn_fwd_kernel, grid=(n_heads // HEADS,),
        in_specs=[head, head, head, fixed(seq, 1), fixed(seq, 1), gain, gain, fixed(seq, HEAD_DIM), fixed(seq, HEAD_DIM)],
        out_specs=[head, head, head, lse],
        out_shape=[bf_shape(seq, width)] * 3 + [f32_shape(n_heads, 1, seq)],
        cost_estimate=cost(4 * seq * seq * width, 16 * seq * width, seq * seq * n_heads // 2),
        compiler_params=limit(40), name="attention_fwd",
    )(q_raw, k_raw, v_val, q_inv, k_inv, g_query.reshape(1, width), g_key.reshape(1, width), cos_t, sin_t)


def attn_bwd_call(q_bf, k_bf, v_val, d_attn, lse_all, dep):
    seq, width = q_bf.shape
    n_heads = width // HEAD_DIM
    head, lse = attn_specs(seq, 1)
    return pl.pallas_call(
        attn_bwd_kernel, grid=(n_heads,),
        in_specs=[head, head, head, head, lse, ANY_SPEC],
        out_specs=[head] * 3, out_shape=[bf_shape(seq, width)] * 3,
        scratch_shapes=[pltpu.VMEM((seq, HEAD_DIM), jnp.float32)] * 2,
        cost_estimate=cost(10 * seq * seq * width, 14 * seq * width, seq * seq * n_heads // 2),
        compiler_params=limit(40), name="attention_bwd",
    )(q_bf, k_bf, v_val, d_attn, lse_all, dep)


def out_kernel(a_ref, w_ref, x_ref, dep_ref, y_ref):
    y_ref[...] = (x_ref[...].astype(jnp.float32) + mm(a_ref[...], w_ref[...])).astype(jnp.bfloat16)


def out_call(attended, w_out, x_seq, dep):
    rows, width = x_seq.shape
    o_col = pl.BlockSpec((rows, WIDE), lambda i: (0, i))
    return pl.pallas_call(
        out_kernel, grid=(width // WIDE,),
        in_specs=[fixed(rows, width), pl.BlockSpec((width, WIDE), lambda i: (0, i)), o_col, ANY_SPEC],
        out_specs=o_col, out_shape=bf_shape(rows, width),
        cost_estimate=cost(2 * rows * width * width, 2 * width * width + 6 * rows * width),
        compiler_params=limit(32), name="project_out",
    )(attended, w_out, x_seq, dep)


def head_grad_kernel(gy_ref, w_ref, dep_ref, out_ref):
    out_ref[...] = mm_nt(gy_ref[...], w_ref[...]).astype(jnp.bfloat16)


def head_grad_call(gy_seq, w_out, dep):
    rows, width = gy_seq.shape
    return pl.pallas_call(
        head_grad_kernel, grid=(width // WIDE,),
        in_specs=[fixed(rows, width), pl.BlockSpec((WIDE, width), lambda i: (i, 0)), ANY_SPEC],
        out_specs=pl.BlockSpec((rows, WIDE), lambda i: (0, i)), out_shape=bf_shape(rows, width),
        cost_estimate=cost(2 * rows * width * width, 2 * width * width + 4 * rows * width),
        compiler_params=limit(32), name="head_grad",
    )(gy_seq, w_out, dep)


def copy_kernel(in_ref, dep_ref, out_ref):
    out_ref[...] = in_ref[...]


def copy_call(values, dep):
    blk = pl.BlockSpec((1,) + values.shape[1:], lambda i: (i, 0, 0))
    return pl.pallas_call(
        copy_kernel, grid=(values.shape[0],), in_specs=[blk, ANY_SPEC], out_specs=blk,
        out_shape=jax.ShapeDtypeStruct(values.shape, values.dtype),
        cost_estimate=cost(0, 4 * values.size), compiler_params=limit(16), name="store_rows",
    )(values, dep)


def hid_grad_kernel(dq_ref, dk_ref, dv_ref, wq_ref, wk_ref, wv_ref, dep_ref, out_ref):
    out_ref[...] = mm_nt(dq_ref[...], wq_ref[...]) + mm_nt(dk_ref[...], wk_ref[...]) + mm_nt(dv_ref[...], wv_ref[...])


def hid_grad_call(dq_raw, dk_raw, dv_bf, w_query, w_key, w_value, dep):
    rows, width = dq_raw.shape
    w_row = pl.BlockSpec((N_BLK, width), lambda i: (i, 0))
    return pl.pallas_call(
        hid_grad_kernel, grid=(width // N_BLK,),
        in_specs=[fixed(rows, width)] * 3 + [w_row] * 3 + [ANY_SPEC],
        out_specs=pl.BlockSpec((rows, N_BLK), lambda i: (0, i)), out_shape=f32_shape(rows, width),
        cost_estimate=cost(6 * rows * width * width, 6 * width * width + 10 * rows * width),
        compiler_params=limit(40), name="hidden_grad",
    )(dq_raw, dk_raw, dv_bf, w_query, w_key, w_value, dep)


def x_grad_kernel(dh_ref, x_ref, gy_ref, gain_ref, gx_ref, gsum_ref):
    x_f = x_ref[...].astype(jnp.float32)
    inv_rms = lax.rsqrt(jnp.mean(x_f * x_f, axis=-1, keepdims=True) + NORM_EPS)
    hat = x_f * inv_rms
    d_hid = dh_ref[...]

    @pl.when(pl.program_id(0) == 0)
    def _():
        gsum_ref[...] = jnp.zeros_like(gsum_ref)

    gsum_ref[...] += jnp.sum(d_hid * hat, axis=0, keepdims=True)
    d_nrm = d_hid * gain_ref[...].astype(jnp.float32)
    d_x = inv_rms * (d_nrm - hat * jnp.mean(d_nrm * hat, axis=-1, keepdims=True))
    gx_ref[...] = (gy_ref[...].astype(jnp.float32) + d_x).astype(jnp.bfloat16)


def x_grad_call(d_hid, x_seq, gy_seq, gain):
    rows, width = x_seq.shape
    row_blk = pl.BlockSpec((128, width), lambda i: (i, 0))
    vec = pl.BlockSpec((1, width), lambda i: (0, 0))
    return pl.pallas_call(
        x_grad_kernel, grid=(rows // 128,),
        in_specs=[row_blk, row_blk, row_blk, vec], out_specs=[row_blk, vec],
        out_shape=[bf_shape(rows, width), f32_shape(1, width)],
        cost_estimate=cost(12 * rows * width, 10 * rows * width), compiler_params=limit(16), name="input_grad",
    )(d_hid, x_seq, gy_seq, gain.reshape(1, width))


def weight_kernel(idx_ref, la_ref, lb_ref, ra_ref, rb_ref, dep_ref, xl_ref, yr_ref, kl_ref, kr_ref):
    step = pl.program_id(0)
    y_bit, x_bit = step // 2, lax.rem(step, 2)
    half = kl_ref.shape[-1]
    for lo, (near, far, pick, slot) in ((0, (kl_ref, xl_ref, x_bit, y_bit)), (half, (kr_ref, yr_ref, y_bit, x_bit))):
        part = mm_tn(la_ref[...], ra_ref[:, lo:lo + half]) + mm_tn(lb_ref[...], rb_ref[:, lo:lo + half])

        @pl.when(pick == 0)
        def _():
            near[pl.ds(slot, 1)] = part[None]

        @pl.when(pick == 1)
        def _():
            far[pl.ds(slot, 1)] = part[None]


def weight_call(idx, left_mine, left_peer, right_mine, right_peer, dep):
    rows, width = left_mine.shape
    blk = width // 8
    left = pl.BlockSpec((rows, blk), lambda i, idx_ref: (0, idx_ref[i]))
    right = pl.BlockSpec((rows, width), lambda i, idx_ref: (0, 0), pipeline_mode=pl.Buffered(1))
    out = pl.BlockSpec((2, blk, width // 2), lambda i, idx_ref: (0, 0, 0))
    return pl.pallas_call(
        weight_kernel,
        grid_spec=pltpu.PrefetchScalarGridSpec(
            num_scalar_prefetch=1, grid=(4,),
            in_specs=[left, left, right, right, ANY_SPEC], out_specs=[out] * 4),
        out_shape=[f32_shape(2, blk, width // 2)] * 4,
        cost_estimate=cost(4 * rows * width * width // 2, 12 * rows * width + 2 * width * width),
        compiler_params=limit(48), name="weight_grad",
    )(idx, left_mine, left_peer, right_mine, right_peer, dep)


def merge_kernel(kl_ref, rl_ref, kr_ref, rr_ref, dep_ref, stay_l, away_l, stay_r, away_r):
    stay_l[...] = kl_ref[0] + rl_ref[0]
    away_l[...] = kl_ref[1] + rl_ref[1]
    stay_r[...] = kr_ref[0] + rr_ref[0]
    away_r[...] = kr_ref[1] + rr_ref[1]


def merge_call(keep_l, recv_l, keep_r, recv_r, dep):
    _, rows, cols = keep_l.shape
    inp = pl.BlockSpec((2, 64, cols), lambda i: (0, i, 0))
    out = pl.BlockSpec((64, cols), lambda i: (i, 0))
    return pl.pallas_call(
        merge_kernel, grid=(rows // 64,), in_specs=[inp] * 4 + [ANY_SPEC], out_specs=[out] * 4,
        out_shape=[f32_shape(rows, cols)] * 4,
        cost_estimate=cost(4 * rows * cols, 48 * rows * cols), compiler_params=limit(16), name="merge",
    )(keep_l, recv_l, keep_r, recv_r, dep)


def final_kernel(sl_ref, rl_ref, sr_ref, rr_ref, dep_ref, out_ref):
    half = sl_ref.shape[-1]
    out_ref[:, :half] = sl_ref[...] + rl_ref[...]
    out_ref[:, half:] = sr_ref[...] + rr_ref[...]


def final_call(stay_l, recv_l, stay_r, recv_r, dep):
    rows, cols = stay_l.shape
    inp = pl.BlockSpec((64, cols), lambda i: (i, 0))
    return pl.pallas_call(
        final_kernel, grid=(rows // 64,), in_specs=[inp] * 4 + [ANY_SPEC],
        out_specs=pl.BlockSpec((64, 2 * cols), lambda i: (i, 0)), out_shape=f32_shape(rows, 2 * cols),
        cost_estimate=cost(2 * rows * cols, 24 * rows * cols), compiler_params=limit(16), name="final_add",
    )(stay_l, recv_l, stay_r, recv_r, dep)


def unnorm_kernel(dq_ref, raw_ref, inv_ref, gain_ref, cos_ref, sin_ref, dep_ref, out_ref, gsum_ref, dn_s, hat_s):
    blk, width = raw_ref.shape
    cos_t, sin_t = cos_ref[...], -sin_ref[...]
    inv_rms = inv_ref[...]

    @pl.when(pl.program_id(0) == 0)
    def _():
        gsum_ref[...] = jnp.zeros_like(gsum_ref)

    acc = jnp.zeros((blk, HEAD_DIM), jnp.float32)
    for head in range(width // HEAD_DIM):
        cols = slice(head * HEAD_DIM, (head + 1) * HEAD_DIM)
        d_out = rotate(dq_ref[:, cols].astype(jnp.float32), cos_t, sin_t)
        hat = raw_ref[:, cols] * inv_rms
        gsum_ref[:, cols] += jnp.sum(d_out * hat, axis=0, keepdims=True)
        d_nrm = d_out * gain_ref[:, cols].astype(jnp.float32)
        acc += d_nrm * hat
        dn_s[:, cols] = d_nrm
        hat_s[:, cols] = hat
    mean = jnp.sum(acc, axis=-1, keepdims=True) * (1.0 / width)
    out_ref[...] = (inv_rms * (dn_s[...] - hat_s[...] * mean)).astype(jnp.bfloat16)


def unnorm_call(d_rot, raw, inv_rms, gain, cos_t, sin_t, dep):
    rows, width = raw.shape
    blk = 128
    row_blk = pl.BlockSpec((blk, width), lambda i: (i, 0))
    vec = pl.BlockSpec((1, width), lambda i: (0, 0))
    tab = pl.BlockSpec((blk, HEAD_DIM), lambda i: (i, 0))
    return pl.pallas_call(
        unnorm_kernel, grid=(rows // blk,),
        in_specs=[row_blk, row_blk, pl.BlockSpec((blk, 1), lambda i: (i, 0)), vec, tab, tab, ANY_SPEC],
        out_specs=[row_blk, vec],
        out_shape=[jax.ShapeDtypeStruct((rows, width), jnp.bfloat16), jax.ShapeDtypeStruct((1, width), jnp.float32)],
        scratch_shapes=[pltpu.VMEM((blk, width), jnp.float32)] * 2,
        cost_estimate=pl.CostEstimate(flops=rows * width * 12, bytes_accessed=rows * width * 8, transcendentals=0),
        compiler_params=limit(16), name="unnorm",
    )(d_rot, raw, inv_rms, gain.reshape(1, width), cos_t, sin_t, dep)


def solution(mesh):
    n_sp = mesh.shape['sp']
    swap = functools.partial(lax.all_to_all, axis_name='sp', split_axis=0, concat_axis=0, tiled=True)

    def flip(values, bit):
        return lax.ppermute(values, 'sp', [(dev, dev ^ bit) for dev in range(n_sp)])

    def block_step(x_loc, grad_y, positions, g_norm, w_query, w_key, w_value, w_out, g_query, g_key):
        n_batch, loc_len, width = x_loc.shape
        seq = n_sp * loc_len
        rows = width // n_sp
        me = lax.axis_index('sp')
        idx = me ^ jnp.array([0, 2, 4, 6], jnp.int32)

        def first_hop(parts):
            far_l, far_r, near_l, near_r = parts
            return near_l, flip(far_l, 2), near_r, flip(far_r, 4)

        def second_hop(parts):
            stay_l, away_l, stay_r, away_r = parts
            return stay_l, flip(away_l, 4), stay_r, flip(away_r, 2)

        x_swap, hidden, q_raw, k_raw, v_val, q_inv, k_inv, pos_seq = gather_qkv_call(x_loc, positions, g_norm, w_query, w_key, w_value)
        cos_t, sin_t = rope_tables(pos_seq.reshape(seq))
        x_seq = x_swap.reshape(seq, width)
        grad_y, _ = lax.optimization_barrier((grad_y, q_inv))
        gy_seq = swap(grad_y).reshape(seq, width)
        attended, q_bf, k_bf, lse_all = attn_fwd_call(q_raw, k_raw, v_val, q_inv, k_inv, g_query, g_key, cos_t, sin_t)
        a_peer = flip(attended, 1)
        gy_peer = flip(gy_seq, 1)
        hid_peer = flip(hidden, 1)
        y_seq = out_call(attended, w_out, x_seq, attended)
        y_swap = swap(y_seq.reshape(n_batch, loc_len, width))
        d_attn = head_grad_call(gy_seq, w_out, y_seq)
        part_o = weight_call(idx, attended, a_peer, gy_seq, gy_peer, d_attn)
        hop_o = first_hop(part_o)
        dq_bf, dk_bf, dv_bf = attn_bwd_call(q_bf, k_bf, v_val, d_attn, lse_all, part_o[2])
        dv_peer = flip(dv_bf, 1)
        mrg_o = merge_call(*hop_o, dv_bf)
        fin_o = second_hop(mrg_o)
        part_v = weight_call(idx, hidden, hid_peer, dv_bf, dv_peer, mrg_o[0])
        hop_v = first_hop(part_v)
        dq_raw, gq_sum = unnorm_call(dq_bf, q_raw, q_inv, g_query, cos_t, sin_t, part_v[2])
        dq_peer = flip(dq_raw, 1)
        dk_raw, gk_sum = unnorm_call(dk_bf, k_raw, k_inv, g_key, cos_t, sin_t, dq_raw)
        dk_peer = flip(dk_raw, 1)
        part_q = weight_call(idx, hidden, hid_peer, dq_raw, dq_peer, dk_raw)
        hop_q = first_hop(part_q)
        part_k = weight_call(idx, hidden, hid_peer, dk_raw, dk_peer, part_q[2])
        hop_k = first_hop(part_k)
        d_hid = hid_grad_call(dq_raw, dk_raw, dv_bf, w_query, w_key, w_value, part_k[2])
        gx_seq, gn_sum = x_grad_call(d_hid, x_seq, gy_seq, g_norm)
        gx_swap = swap(gx_seq.reshape(n_batch, loc_len, width))
        gains = jnp.concatenate([gn_sum, gq_sum, gk_sum], axis=0)
        cut = [lax.dynamic_slice_in_dim(gains, (me ^ off) * rows, rows, axis=1) for off in range(n_sp)]
        gain_rows = sum((flip(cut[off], off) for off in range(1, n_sp)), cut[0])
        mrg_v = merge_call(*hop_v, gx_seq)
        fin_v = second_hop(mrg_v)
        mrg_q = merge_call(*hop_q, mrg_v[0])
        fin_q = second_hop(mrg_q)
        y_out = copy_call(y_swap, mrg_q[0])
        mrg_k = merge_call(*hop_k, y_out)
        fin_k = second_hop(mrg_k)
        grad_wo = final_call(*fin_o, mrg_k[0])
        grad_x = copy_call(gx_swap, grad_wo)
        grad_wv = final_call(*fin_v, grad_x)
        grad_wq = final_call(*fin_q, grad_wv)
        grad_wk = final_call(*fin_k, grad_wq)
        return (y_out, grad_x, gain_rows[0], grad_wq, grad_wk, grad_wv, grad_wo, gain_rows[1], gain_rows[2])

    seq_spec = P('dp', 'sp', None)
    mat_rep = P(None, None)
    vec_rep = P(None)
    row_spec = P(('dp', 'sp'), None)
    vec_spec = P(('dp', 'sp'))
    return jax.shard_map(block_step, mesh=mesh, in_specs=(seq_spec, seq_spec, P('dp', 'sp'), vec_rep, mat_rep, mat_rep, mat_rep, mat_rep, vec_rep, vec_rep), out_specs=(seq_spec, seq_spec, vec_spec, row_spec, row_spec, row_spec, row_spec, vec_spec, vec_spec), check_vma=False)
```

```python
import functools
import jax
import jax.numpy as jnp
from jax import lax
from jax.experimental import pallas as pl
from jax.experimental.pallas import tpu as pltpu
from jax.sharding import PartitionSpec as P

HEAD_DIM = 128
NORM_EPS = 1e-5
ROPE_BASE = 10000.0
NEG_BIG = -1e30
Q_BLK = 256
LOG2E = 1.4426950408889634


def mm(lhs, rhs):
    return lax.dot_general(lhs, rhs, (((1,), (0,)), ((), ())), preferred_element_type=jnp.float32)


def mm_nt(lhs, rhs):
    return lax.dot_general(lhs, rhs, (((1,), (1,)), ((), ())), preferred_element_type=jnp.float32)


def mm_tn(lhs, rhs):
    return lax.dot_general(lhs, rhs, (((0,), (0,)), ((), ())), preferred_element_type=jnp.float32)


def rope_tables(positions):
    half_dim = HEAD_DIM // 2
    inv_freq = ROPE_BASE ** (-jnp.arange(half_dim, dtype=jnp.float32) * (2.0 / HEAD_DIM))
    angles = positions.astype(jnp.float32)[..., None] * inv_freq
    cos_h, sin_h = jnp.cos(angles), jnp.sin(angles)
    return jnp.concatenate([cos_h, cos_h], axis=-1), jnp.concatenate([-sin_h, sin_h], axis=-1)


def rotate(values, cos_t, sin_t):
    return values * cos_t + pltpu.roll(values, HEAD_DIM // 2, 1) * sin_t


ANY_SPEC = pl.BlockSpec(memory_space=pltpu.HBM)
N_BLK = 256
MIB = 1024 * 1024
VMEM_MIB = 63
HEADS = 2
WIDE = 512


def bf_shape(*dims):
    return jax.ShapeDtypeStruct(dims, jnp.bfloat16)


def f32_shape(*dims):
    return jax.ShapeDtypeStruct(dims, jnp.float32)


def cost(flops, bytes_moved, exps=0):
    return pl.CostEstimate(flops=flops, bytes_accessed=bytes_moved, transcendentals=exps)


def limit(mib):
    return pltpu.CompilerParams(vmem_limit_bytes=max(mib, VMEM_MIB) * MIB)


def fixed(*dims):
    return pl.BlockSpec(dims, lambda i: (0,) * len(dims), pipeline_mode=pl.Buffered(1))


def partner_of(me, off):
    flipped = me
    for bit in (1, 2, 4):
        if off & bit:
            flipped = flipped + bit - 2 * bit * ((me // bit) % 2)
    return flipped


def gather_qkv_kernel(x_ref, pos_ref, gain_ref, wq_ref, wk_ref, wv_ref, xs_ref, hid_ref, q_ref, k_ref, v_ref, qinv_ref, kinv_ref, pos_out,
                      x_s, pos_s, wq_s, wk_s, wv_s, hid_s, q_s, k_s, v_s, send_sem, recv_sem, psend_sem, precv_sem, w_sem, own_sem, x_out_sem, out_sem):
    n_sp, tok, width = x_ref.shape
    me = lax.axis_index('sp')
    pair = 2 * tok
    barrier = pltpu.get_barrier_semaphore()
    for off in range(1, n_sp):
        pl.semaphore_signal(barrier, inc=1, device_id={'sp': partner_of(me, off)}, device_id_type=pl.DeviceIdType.MESH)
    pl.semaphore_wait(barrier, n_sp - 1)

    copies, pos_copies = [], []
    for off in range(n_sp):
        peer = partner_of(me, off)
        if off == 0:
            copies.append(pltpu.make_async_copy(x_ref.at[me], x_s.at[me], own_sem.at[0]))
            pos_copies.append(pltpu.make_async_copy(pos_ref.at[me], pos_s.at[me], own_sem.at[1]))
        else:
            pos_copies.append(pltpu.make_async_remote_copy(
                src_ref=pos_ref.at[peer], dst_ref=pos_s.at[me], send_sem=psend_sem.at[off], recv_sem=precv_sem.at[off],
                device_id={'sp': peer}, device_id_type=pl.DeviceIdType.MESH))
            copies.append(pltpu.make_async_remote_copy(
                src_ref=x_ref.at[peer], dst_ref=x_s.at[me], send_sem=send_sem.at[off], recv_sem=recv_sem.at[off],
                device_id={'sp': peer}, device_id_type=pl.DeviceIdType.MESH))
        pos_copies[-1].start()
        copies[-1].start()
    loads = [pltpu.make_async_copy(src, dst, w_sem.at[i]) for i, (src, dst) in enumerate(((wq_ref, wq_s), (wk_ref, wk_s), (wv_ref, wv_s)))]
    for load in loads:
        load.start()

    outs = []
    for step in range(n_sp // 2):
        slot = step % 2
        chip = partner_of(me, 2 * step) // 2
        if step == 0:
            copies[0].wait()
        else:
            copies[2 * step].wait_recv()
        copies[2 * step + 1].wait_recv()
        rows = pl.ds(pl.multiple_of(chip * pair, pair), pair)
        if step >= 2:
            for out in outs[step - 2]:
                out.wait()
        for part in range(2):
            x_f = x_s[2 * chip + part].astype(jnp.float32)
            inv_rms = lax.rsqrt(jnp.mean(x_f * x_f, axis=-1, keepdims=True) + NORM_EPS)
            hid_s[slot, part * tok:(part + 1) * tok, :] = (x_f * inv_rms * gain_ref[...].astype(jnp.float32)).astype(jnp.bfloat16)
        if step == 0:
            for load in loads:
                load.wait()

        early = [pltpu.make_async_copy(hid_s.at[slot], hid_ref.at[rows], out_sem.at[slot, 3])]
        for part in range(2):
            early.append(pltpu.make_async_copy(x_s.at[2 * chip + part], xs_ref.at[2 * chip + part], x_out_sem.at[2 * step + part]))
        for out in early:
            out.start()

        def columns(blk, sums):
            cols = pl.ds(pl.multiple_of(blk * WIDE, WIDE), WIDE)
            hid = hid_s[slot]
            new_sums = []
            for w_s, dst, total in ((wq_s, q_s, sums[0]), (wk_s, k_s, sums[1])):
                raw = mm(hid, w_s[:, cols])
                dst[slot, :, cols] = raw
                for lo in range(0, WIDE, 128):
                    total = total + raw[:, lo:lo + 128] * raw[:, lo:lo + 128]
                new_sums.append(total)
            v_s[slot, :, cols] = mm(hid, wv_s[:, cols]).astype(jnp.bfloat16)
            return tuple(new_sums)

        zero = jnp.zeros((pair, 128), jnp.float32)
        sums = lax.fori_loop(0, width // WIDE, columns, (zero, zero))
        for total, inv_ref in zip(sums, (qinv_ref, kinv_ref)):
            inv_ref[rows, :] = lax.rsqrt(jnp.sum(total, axis=-1, keepdims=True) * (1.0 / width) + NORM_EPS)
        late = [pltpu.make_async_copy(src.at[slot], dst.at[rows], out_sem.at[slot, i])
                for i, (src, dst) in enumerate(((q_s, q_ref), (k_s, k_ref), (v_s, v_ref)))]
        for out in late:
            out.start()
        outs.append(early + late)
    for group in outs[-2:]:
        for out in group:
            out.wait()
    pos_copies[0].wait()
    for off in range(1, n_sp):
        pos_copies[off].wait()
        copies[off].wait_send()
    pos_out[...] = pos_s[...]


def gather_qkv_call(x_loc, positions, gain, w_query, w_key, w_value):
    n_sp, tok, width = x_loc.shape
    rows, pair = n_sp * tok, 2 * tok
    hbm = pl.BlockSpec(memory_space=pltpu.HBM)
    vmem = pl.BlockSpec(memory_space=pltpu.VMEM)
    dma = pltpu.SemaphoreType.DMA
    return pl.pallas_call(
        gather_qkv_kernel,
        in_specs=[hbm, hbm, vmem, hbm, hbm, hbm],
        out_specs=[hbm] * 5 + [vmem] * 3,
        out_shape=[bf_shape(n_sp, tok, width), bf_shape(rows, width), f32_shape(rows, width), f32_shape(rows, width), bf_shape(rows, width),
                   f32_shape(rows, 1), f32_shape(rows, 1), jax.ShapeDtypeStruct((n_sp, 1, tok), jnp.int32)],
        scratch_shapes=[
            pltpu.VMEM((n_sp, tok, width), jnp.bfloat16), pltpu.VMEM((n_sp, 1, tok), jnp.int32)]
        + [pltpu.VMEM((width, width), jnp.bfloat16)] * 3
        + [pltpu.VMEM((2, pair, width), jnp.bfloat16), pltpu.VMEM((2, pair, width), jnp.float32), pltpu.VMEM((2, pair, width), jnp.float32), pltpu.VMEM((2, pair, width), jnp.bfloat16)]
        + [dma((n_sp,)), dma((n_sp,)), dma((n_sp,)), dma((n_sp,)), dma((3,)), dma((2,)), dma((n_sp,)), dma((2, 4))],
        cost_estimate=cost(6 * rows * width * width, 6 * width * width + 14 * rows * width),
        compiler_params=pltpu.CompilerParams(vmem_limit_bytes=VMEM_MIB * MIB, collective_id=0, has_side_effects=True),
        name="gather_qkv",
    )(x_loc, positions.reshape(n_sp, 1, tok), gain.reshape(1, width), w_query, w_key, w_value)


def rope_heads(q1_ref, k1_ref, qinv_ref, kinv_ref, gq_ref, gk_ref, cos_ref, sin_ref, q_s, k_s, cols):
    cos_t, sin_t = cos_ref[...], sin_ref[...]
    q_s[:, cols] = rotate(q1_ref[:, cols] * qinv_ref[...] * gq_ref[:, cols].astype(jnp.float32), cos_t, sin_t).astype(jnp.bfloat16)
    k_s[:, cols] = rotate(k1_ref[:, cols] * kinv_ref[...] * gk_ref[:, cols].astype(jnp.float32), cos_t, sin_t).astype(jnp.bfloat16)


def masked_scores(keys, q_blk, q_lo):
    scores = mm_nt(keys, q_blk)
    edge = scores[q_lo:, :]
    key_pos = lax.broadcasted_iota(jnp.int32, edge.shape, 0)
    q_pos = lax.broadcasted_iota(jnp.int32, edge.shape, 1)
    edge = jnp.where(q_pos >= key_pos, edge, NEG_BIG)
    return edge if q_lo == 0 else jnp.concatenate([scores[:q_lo, :], edge], axis=0)


def head_cols(head):
    return slice(head * HEAD_DIM, (head + 1) * HEAD_DIM)


def attn_fwd_kernel(q1_ref, k1_ref, v_ref, qinv_ref, kinv_ref, gq_ref, gk_ref, cos_ref, sin_ref, a_ref, q_s, k_s, lse_ref):
    seq = q1_ref.shape[0]
    to_log2 = HEAD_DIM ** -0.5 * LOG2E
    for head in range(HEADS):
        rope_heads(q1_ref, k1_ref, qinv_ref, kinv_ref, gq_ref, gk_ref, cos_ref, sin_ref, q_s, k_s, head_cols(head))
    v_t = [v_ref[:, head_cols(head)].T for head in range(HEADS)]
    for blk in range(seq // Q_BLK):
        q_lo, k_len = blk * Q_BLK, (blk + 1) * Q_BLK
        scores = [masked_scores(k_s[:k_len, head_cols(h)], q_s[q_lo:k_len, head_cols(h)], q_lo) for h in range(HEADS)]
        for head in range(HEADS):
            top = jnp.max(scores[head], axis=0, keepdims=True)
            prob = jnp.exp2((scores[head] - top) * to_log2)
            total = jnp.sum(prob, axis=0, keepdims=True)
            out_t = mm(v_t[head][:, :k_len], prob.astype(jnp.bfloat16)) * (1.0 / total)
            a_ref[q_lo:k_len, head_cols(head)] = out_t.T.astype(jnp.bfloat16)
            lse_ref[head, :, q_lo:k_len] = top * to_log2 + jnp.log2(total)


def attn_bwd_kernel(q_ref, k_ref, v_ref, do_ref, lse_ref, dep_ref, dq_ref, dk_ref, dv_ref, dk_s, dv_s):
    seq = q_ref.shape[0]
    scale = HEAD_DIM ** -0.5
    k_t = [k_ref[:, head_cols(head)].T for head in range(1)]
    n_blk = seq // Q_BLK
    for blk in reversed(range(n_blk)):
        q_lo, k_len = blk * Q_BLK, (blk + 1) * Q_BLK
        for head in range(1):
            cols = head_cols(head)
            q_blk = q_ref[q_lo:k_len, cols]
            do_blk = do_ref[q_lo:k_len, cols]
            scores = masked_scores(k_ref[:k_len, cols], q_blk, q_lo)
            prob = jnp.exp2(scores * (scale * LOG2E) - lse_ref[head, :, q_lo:k_len])
            d_prob = mm_nt(v_ref[:k_len, cols], do_blk)
            row_dot = jnp.sum(prob * d_prob, axis=0, keepdims=True)
            ds_bf = (prob * ((d_prob - row_dot) * scale)).astype(jnp.bfloat16)
            dq_t = mm(k_t[head][:, :k_len], ds_bf)
            dq_ref[q_lo:k_len, cols] = dq_t.T.astype(jnp.bfloat16)
            dv_part = mm(prob.astype(jnp.bfloat16), do_blk)
            dk_part = mm(ds_bf, q_blk)
            if blk == n_blk - 1:
                dv_s[:, cols] = dv_part
                dk_s[:, cols] = dk_part
            else:
                dv_s[:k_len, cols] += dv_part
                dk_s[:k_len, cols] += dk_part
    dv_ref[...] = dv_s[...].astype(jnp.bfloat16)
    dk_ref[...] = dk_s[...].astype(jnp.bfloat16)


def attn_specs(seq, heads):
    head = pl.BlockSpec((seq, heads * HEAD_DIM), lambda h: (0, h))
    lse = pl.BlockSpec((heads, 1, seq), lambda h: (h, 0, 0))
    return head, lse


def attn_fwd_call(q_raw, k_raw, v_val, q_inv, k_inv, g_query, g_key, cos_t, sin_t):
    seq, width = q_raw.shape
    n_heads = width // HEAD_DIM
    head, lse = attn_specs(seq, HEADS)
    gain = pl.BlockSpec((1, HEADS * HEAD_DIM), lambda h: (0, h))
    return pl.pallas_call(
        attn_fwd_kernel, grid=(n_heads // HEADS,),
        in_specs=[head, head, head, fixed(seq, 1), fixed(seq, 1), gain, gain, fixed(seq, HEAD_DIM), fixed(seq, HEAD_DIM)],
        out_specs=[head, head, head, lse],
        out_shape=[bf_shape(seq, width)] * 3 + [f32_shape(n_heads, 1, seq)],
        cost_estimate=cost(4 * seq * seq * width, 16 * seq * width, seq * seq * n_heads // 2),
        compiler_params=limit(40), name="attention_fwd",
    )(q_raw, k_raw, v_val, q_inv, k_inv, g_query.reshape(1, width), g_key.reshape(1, width), cos_t, sin_t)


def attn_bwd_call(q_bf, k_bf, v_val, d_attn, lse_all, dep):
    seq, width = q_bf.shape
    n_heads = width // HEAD_DIM
    head, lse = attn_specs(seq, 1)
    return pl.pallas_call(
        attn_bwd_kernel, grid=(n_heads,),
        in_specs=[head, head, head, head, lse, ANY_SPEC],
        out_specs=[head] * 3, out_shape=[bf_shape(seq, width)] * 3,
        scratch_shapes=[pltpu.VMEM((seq, HEAD_DIM), jnp.float32)] * 2,
        cost_estimate=cost(10 * seq * seq * width, 14 * seq * width, seq * seq * n_heads // 2),
        compiler_params=limit(40), name="attention_bwd",
    )(q_bf, k_bf, v_val, d_attn, lse_all, dep)


def out_kernel(a_ref, w_ref, x_ref, dep_ref, y_ref):
    y_ref[...] = (x_ref[...].astype(jnp.float32) + mm(a_ref[...], w_ref[...])).astype(jnp.bfloat16)


def out_call(attended, w_out, x_seq, dep):
    rows, width = x_seq.shape
    o_col = pl.BlockSpec((rows, WIDE), lambda i: (0, i))
    return pl.pallas_call(
        out_kernel, grid=(width // WIDE,),
        in_specs=[fixed(rows, width), pl.BlockSpec((width, WIDE), lambda i: (0, i)), o_col, ANY_SPEC],
        out_specs=o_col, out_shape=bf_shape(rows, width),
        cost_estimate=cost(2 * rows * width * width, 2 * width * width + 6 * rows * width),
        compiler_params=limit(32), name="project_out",
    )(attended, w_out, x_seq, dep)


def head_grad_kernel(gy_ref, w_ref, dep_ref, out_ref):
    out_ref[...] = mm_nt(gy_ref[...], w_ref[...]).astype(jnp.bfloat16)


def head_grad_call(gy_seq, w_out, dep):
    rows, width = gy_seq.shape
    return pl.pallas_call(
        head_grad_kernel, grid=(width // N_BLK,),
        in_specs=[fixed(rows, width), pl.BlockSpec((N_BLK, width), lambda i: (i, 0)), ANY_SPEC],
        out_specs=pl.BlockSpec((rows, N_BLK), lambda i: (0, i)), out_shape=bf_shape(rows, width),
        cost_estimate=cost(2 * rows * width * width, 2 * width * width + 4 * rows * width),
        compiler_params=limit(32), name="head_grad",
    )(gy_seq, w_out, dep)


def copy_kernel(in_ref, dep_ref, out_ref):
    out_ref[...] = in_ref[...]


def copy_call(values, dep):
    blk = pl.BlockSpec((1,) + values.shape[1:], lambda i: (i, 0, 0))
    return pl.pallas_call(
        copy_kernel, grid=(values.shape[0],), in_specs=[blk, ANY_SPEC], out_specs=blk,
        out_shape=jax.ShapeDtypeStruct(values.shape, values.dtype),
        cost_estimate=cost(0, 4 * values.size), compiler_params=limit(16), name="store_rows",
    )(values, dep)


def hid_grad_kernel(dq_ref, dk_ref, dv_ref, wq_ref, wk_ref, wv_ref, dep_ref, out_ref):
    out_ref[...] = mm_nt(dq_ref[...], wq_ref[...]) + mm_nt(dk_ref[...], wk_ref[...]) + mm_nt(dv_ref[...], wv_ref[...])


def hid_grad_call(dq_raw, dk_raw, dv_bf, w_query, w_key, w_value, dep):
    rows, width = dq_raw.shape
    w_row = pl.BlockSpec((N_BLK, width), lambda i: (i, 0))
    return pl.pallas_call(
        hid_grad_kernel, grid=(width // N_BLK,),
        in_specs=[fixed(rows, width)] * 3 + [w_row] * 3 + [ANY_SPEC],
        out_specs=pl.BlockSpec((rows, N_BLK), lambda i: (0, i)), out_shape=f32_shape(rows, width),
        cost_estimate=cost(6 * rows * width * width, 6 * width * width + 10 * rows * width),
        compiler_params=limit(40), name="hidden_grad",
    )(dq_raw, dk_raw, dv_bf, w_query, w_key, w_value, dep)


def x_grad_kernel(dh_ref, x_ref, gy_ref, gain_ref, gx_ref, gsum_ref):
    x_f = x_ref[...].astype(jnp.float32)
    inv_rms = lax.rsqrt(jnp.mean(x_f * x_f, axis=-1, keepdims=True) + NORM_EPS)
    hat = x_f * inv_rms
    d_hid = dh_ref[...]

    @pl.when(pl.program_id(0) == 0)
    def _():
        gsum_ref[...] = jnp.zeros_like(gsum_ref)

    gsum_ref[...] += jnp.sum(d_hid * hat, axis=0, keepdims=True)
    d_nrm = d_hid * gain_ref[...].astype(jnp.float32)
    d_x = inv_rms * (d_nrm - hat * jnp.mean(d_nrm * hat, axis=-1, keepdims=True))
    gx_ref[...] = (gy_ref[...].astype(jnp.float32) + d_x).astype(jnp.bfloat16)


def x_grad_call(d_hid, x_seq, gy_seq, gain):
    rows, width = x_seq.shape
    row_blk = pl.BlockSpec((128, width), lambda i: (i, 0))
    vec = pl.BlockSpec((1, width), lambda i: (0, 0))
    return pl.pallas_call(
        x_grad_kernel, grid=(rows // 128,),
        in_specs=[row_blk, row_blk, row_blk, vec], out_specs=[row_blk, vec],
        out_shape=[bf_shape(rows, width), f32_shape(1, width)],
        cost_estimate=cost(12 * rows * width, 10 * rows * width), compiler_params=limit(16), name="input_grad",
    )(d_hid, x_seq, gy_seq, gain.reshape(1, width))


def weight_kernel(idx_ref, la_ref, lb_ref, ra_ref, rb_ref, dep_ref, xl_ref, yr_ref, kl_ref, kr_ref):
    step = pl.program_id(0)
    y_bit, x_bit = step // 2, lax.rem(step, 2)
    half = kl_ref.shape[-1]
    for lo, (near, far, pick, slot) in ((0, (kl_ref, xl_ref, x_bit, y_bit)), (half, (kr_ref, yr_ref, y_bit, x_bit))):
        part = mm_tn(la_ref[...], ra_ref[:, lo:lo + half]) + mm_tn(lb_ref[...], rb_ref[:, lo:lo + half])

        @pl.when(pick == 0)
        def _():
            near[pl.ds(slot, 1)] = part[None]

        @pl.when(pick == 1)
        def _():
            far[pl.ds(slot, 1)] = part[None]


def weight_call(idx, left_mine, left_peer, right_mine, right_peer, dep):
    rows, width = left_mine.shape
    blk = width // 8
    left = pl.BlockSpec((rows, blk), lambda i, idx_ref: (0, idx_ref[i]))
    right = pl.BlockSpec((rows, width), lambda i, idx_ref: (0, 0), pipeline_mode=pl.Buffered(1))
    out = pl.BlockSpec((2, blk, width // 2), lambda i, idx_ref: (0, 0, 0))
    return pl.pallas_call(
        weight_kernel,
        grid_spec=pltpu.PrefetchScalarGridSpec(
            num_scalar_prefetch=1, grid=(4,),
            in_specs=[left, left, right, right, ANY_SPEC], out_specs=[out] * 4),
        out_shape=[f32_shape(2, blk, width // 2)] * 4,
        cost_estimate=cost(4 * rows * width * width // 2, 12 * rows * width + 2 * width * width),
        compiler_params=limit(48), name="weight_grad",
    )(idx, left_mine, left_peer, right_mine, right_peer, dep)


def merge_kernel(kl_ref, rl_ref, kr_ref, rr_ref, dep_ref, stay_l, away_l, stay_r, away_r):
    stay_l[...] = kl_ref[0] + rl_ref[0]
    away_l[...] = kl_ref[1] + rl_ref[1]
    stay_r[...] = kr_ref[0] + rr_ref[0]
    away_r[...] = kr_ref[1] + rr_ref[1]


def merge_call(keep_l, recv_l, keep_r, recv_r, dep):
    _, rows, cols = keep_l.shape
    inp = pl.BlockSpec((2, 64, cols), lambda i: (0, i, 0))
    out = pl.BlockSpec((64, cols), lambda i: (i, 0))
    return pl.pallas_call(
        merge_kernel, grid=(rows // 64,), in_specs=[inp] * 4 + [ANY_SPEC], out_specs=[out] * 4,
        out_shape=[f32_shape(rows, cols)] * 4,
        cost_estimate=cost(4 * rows * cols, 48 * rows * cols), compiler_params=limit(16), name="merge",
    )(keep_l, recv_l, keep_r, recv_r, dep)


def final_kernel(sl_ref, rl_ref, sr_ref, rr_ref, dep_ref, out_ref):
    half = sl_ref.shape[-1]
    out_ref[:, :half] = sl_ref[...] + rl_ref[...]
    out_ref[:, half:] = sr_ref[...] + rr_ref[...]


def final_call(stay_l, recv_l, stay_r, recv_r, dep):
    rows, cols = stay_l.shape
    inp = pl.BlockSpec((64, cols), lambda i: (i, 0))
    return pl.pallas_call(
        final_kernel, grid=(rows // 64,), in_specs=[inp] * 4 + [ANY_SPEC],
        out_specs=pl.BlockSpec((64, 2 * cols), lambda i: (i, 0)), out_shape=f32_shape(rows, 2 * cols),
        cost_estimate=cost(2 * rows * cols, 24 * rows * cols), compiler_params=limit(16), name="final_add",
    )(stay_l, recv_l, stay_r, recv_r, dep)


def unnorm_kernel(dq_ref, raw_ref, inv_ref, gain_ref, cos_ref, sin_ref, dep_ref, out_ref, gsum_ref, dn_s, hat_s):
    blk, width = raw_ref.shape
    cos_t, sin_t = cos_ref[...], -sin_ref[...]
    inv_rms = inv_ref[...]

    @pl.when(pl.program_id(0) == 0)
    def _():
        gsum_ref[...] = jnp.zeros_like(gsum_ref)

    acc = jnp.zeros((blk, HEAD_DIM), jnp.float32)
    for head in range(width // HEAD_DIM):
        cols = slice(head * HEAD_DIM, (head + 1) * HEAD_DIM)
        d_out = rotate(dq_ref[:, cols].astype(jnp.float32), cos_t, sin_t)
        hat = raw_ref[:, cols] * inv_rms
        gsum_ref[:, cols] += jnp.sum(d_out * hat, axis=0, keepdims=True)
        d_nrm = d_out * gain_ref[:, cols].astype(jnp.float32)
        acc += d_nrm * hat
        dn_s[:, cols] = d_nrm
        hat_s[:, cols] = hat
    mean = jnp.sum(acc, axis=-1, keepdims=True) * (1.0 / width)
    out_ref[...] = (inv_rms * (dn_s[...] - hat_s[...] * mean)).astype(jnp.bfloat16)


def unnorm_call(d_rot, raw, inv_rms, gain, cos_t, sin_t, dep):
    rows, width = raw.shape
    blk = 128
    row_blk = pl.BlockSpec((blk, width), lambda i: (i, 0))
    vec = pl.BlockSpec((1, width), lambda i: (0, 0))
    tab = pl.BlockSpec((blk, HEAD_DIM), lambda i: (i, 0))
    return pl.pallas_call(
        unnorm_kernel, grid=(rows // blk,),
        in_specs=[row_blk, row_blk, pl.BlockSpec((blk, 1), lambda i: (i, 0)), vec, tab, tab, ANY_SPEC],
        out_specs=[row_blk, vec],
        out_shape=[jax.ShapeDtypeStruct((rows, width), jnp.bfloat16), jax.ShapeDtypeStruct((1, width), jnp.float32)],
        scratch_shapes=[pltpu.VMEM((blk, width), jnp.float32)] * 2,
        cost_estimate=pl.CostEstimate(flops=rows * width * 12, bytes_accessed=rows * width * 8, transcendentals=0),
        compiler_params=limit(16), name="unnorm",
    )(d_rot, raw, inv_rms, gain.reshape(1, width), cos_t, sin_t, dep)


def solution(mesh):
    n_sp = mesh.shape['sp']
    swap = functools.partial(lax.all_to_all, axis_name='sp', split_axis=0, concat_axis=0, tiled=True)

    def flip(values, bit):
        return lax.ppermute(values, 'sp', [(dev, dev ^ bit) for dev in range(n_sp)])

    def block_step(x_loc, grad_y, positions, g_norm, w_query, w_key, w_value, w_out, g_query, g_key):
        n_batch, loc_len, width = x_loc.shape
        seq = n_sp * loc_len
        rows = width // n_sp
        me = lax.axis_index('sp')
        idx = me ^ jnp.array([0, 2, 4, 6], jnp.int32)

        def first_hop(parts):
            far_l, far_r, near_l, near_r = parts
            return near_l, flip(far_l, 2), near_r, flip(far_r, 4)

        def second_hop(parts):
            stay_l, away_l, stay_r, away_r = parts
            return stay_l, flip(away_l, 4), stay_r, flip(away_r, 2)

        x_swap, hidden, q_raw, k_raw, v_val, q_inv, k_inv, pos_seq = gather_qkv_call(x_loc, positions, g_norm, w_query, w_key, w_value)
        cos_t, sin_t = rope_tables(pos_seq.reshape(seq))
        x_seq = x_swap.reshape(seq, width)
        grad_y, _ = lax.optimization_barrier((grad_y, q_inv))
        gy_seq = swap(grad_y).reshape(seq, width)
        attended, q_bf, k_bf, lse_all = attn_fwd_call(q_raw, k_raw, v_val, q_inv, k_inv, g_query, g_key, cos_t, sin_t)
        a_peer = flip(attended, 1)
        gy_peer = flip(gy_seq, 1)
        hid_peer = flip(hidden, 1)
        y_seq = out_call(attended, w_out, x_seq, attended)
        y_swap = swap(y_seq.reshape(n_batch, loc_len, width))
        d_attn = head_grad_call(gy_seq, w_out, y_seq)
        part_o = weight_call(idx, attended, a_peer, gy_seq, gy_peer, d_attn)
        hop_o = first_hop(part_o)
        dq_bf, dk_bf, dv_bf = attn_bwd_call(q_bf, k_bf, v_val, d_attn, lse_all, part_o[2])
        dv_peer = flip(dv_bf, 1)
        mrg_o = merge_call(*hop_o, dv_bf)
        fin_o = second_hop(mrg_o)
        part_v = weight_call(idx, hidden, hid_peer, dv_bf, dv_peer, mrg_o[0])
        hop_v = first_hop(part_v)
        dq_raw, gq_sum = unnorm_call(dq_bf, q_raw, q_inv, g_query, cos_t, sin_t, part_v[2])
        dq_peer = flip(dq_raw, 1)
        dk_raw, gk_sum = unnorm_call(dk_bf, k_raw, k_inv, g_key, cos_t, sin_t, dq_raw)
        dk_peer = flip(dk_raw, 1)
        part_q = weight_call(idx, hidden, hid_peer, dq_raw, dq_peer, dk_raw)
        hop_q = first_hop(part_q)
        part_k = weight_call(idx, hidden, hid_peer, dk_raw, dk_peer, part_q[2])
        hop_k = first_hop(part_k)
        d_hid = hid_grad_call(dq_raw, dk_raw, dv_bf, w_query, w_key, w_value, part_k[2])
        gx_seq, gn_sum = x_grad_call(d_hid, x_seq, gy_seq, g_norm)
        gx_swap = swap(gx_seq.reshape(n_batch, loc_len, width))
        gains = jnp.concatenate([gn_sum, gq_sum, gk_sum], axis=0)
        cut = [lax.dynamic_slice_in_dim(gains, (me ^ off) * rows, rows, axis=1) for off in range(n_sp)]
        gain_rows = sum((flip(cut[off], off) for off in range(1, n_sp)), cut[0])
        mrg_v = merge_call(*hop_v, gx_seq)
        fin_v = second_hop(mrg_v)
        mrg_q = merge_call(*hop_q, mrg_v[0])
        fin_q = second_hop(mrg_q)
        y_out = copy_call(y_swap, mrg_q[0])
        mrg_k = merge_call(*hop_k, y_out)
        fin_k = second_hop(mrg_k)
        grad_wo = final_call(*fin_o, mrg_k[0])
        grad_x = copy_call(gx_swap, grad_wo)
        grad_wv = final_call(*fin_v, grad_x)
        grad_wq = final_call(*fin_q, grad_wv)
        grad_wk = final_call(*fin_k, grad_wq)
        return (y_out, grad_x, gain_rows[0], grad_wq, grad_wk, grad_wv, grad_wo, gain_rows[1], gain_rows[2])

    seq_spec = P('dp', 'sp', None)
    mat_rep = P(None, None)
    vec_rep = P(None)
    row_spec = P(('dp', 'sp'), None)
    vec_spec = P(('dp', 'sp'))
    return jax.shard_map(block_step, mesh=mesh, in_specs=(seq_spec, seq_spec, P('dp', 'sp'), vec_rep, mat_rep, mat_rep, mat_rep, mat_rep, vec_rep, vec_rep), out_specs=(seq_spec, seq_spec, vec_spec, row_spec, row_spec, row_spec, row_spec, vec_spec, vec_spec), check_vma=False)
```
